32 devices in a mesh: gx: 4 (over y, core), gy: 8 (over z, x).
Axes of the slice: x: 2, y: 2, z: 4, core: 2. Of those that a mesh axis runs over, the one named last changes fastest.
Arguments:
- old_master: float32 [32, 128, 1536], P('gx', 'gy'), may hold values from -3 to 3
- old_first: float32 [32, 128, 1536], P('gx', 'gy'), may hold values from -3 to 3
- old_second: float32 [32, 128, 1536], P('gx', 'gy'), may hold values from 0.01 to 1
- new_grad: bfloat16 [32, 128, 1536], P(('gx', 'gy')), may hold values from -3072 to 3072
- counts: int32 [32, 32], P(None, ('gx', 'gy')), may hold values from 1 to 72, as said below
- old_owner: int32 [32], replicated, may hold values from 0 to 31, each once
- new_owner: int32 [32], replicated, may hold values from 0 to 31, each once
Outputs:
- new_master: float32 [32, 128, 1536], P(('gx', 'gy'))
- new_first: float32 [32, 128, 1536], P(('gx', 'gy'))
- new_second: float32 [32, 128, 1536], P(('gx', 'gy'))
The draws below stay inside these ranges and needn't reach their ends.
Inputs may be any that keep to these rules, and one draw needn't show every extreme that they name: `old_owner`: every number of 0 to 31 appears once. `new_owner`: every number of 0 to 31 appears once. `counts`: every device routed at least one token to every expert.
All inputs are finite; a program needn't handle non-finite values.
Results may differ from the reference program's by a relative error of at most 0.0003.
Values sent between devices are 32-bit elements; how exact they have to be, the bound alone decides.
No kernel may reach another device: no remote copies, remote signals or barrier semaphores. Data moves between devices by JAX's collectives and lax.ppermute only.
A program may use at most 64 MiB of HBM per device.

```python
import math
import jax
import jax.numpy as jnp
from jax import lax

FF = 1536
ROWS = 128
EXPERTS = 32
RANKS = 32


def draw_counts(key, part):
    key_tokens = jax.random.fold_in(key, 11)
    key_skew = jax.random.fold_in(key, 23)
    columns = jnp.arange(RANKS, dtype=jnp.int32)
    ceiling = 6 + 12 * columns // max(RANKS - 1, 1)
    factor = 1 + jax.random.randint(key_skew, (EXPERTS,), 0, 4)
    base = 1 + jax.random.randint(key_tokens, (EXPERTS, RANKS), 0, ceiling[None, :])
    return (base * factor[:, None]).astype(jnp.int32)


def block_scale(stream_key, dims, pieces, low, top_value):
    def one(axis_at, parts):
        heights = jax.random.uniform(jax.random.fold_in(jax.random.fold_in(stream_key, 6), axis_at), (parts,), jnp.float32, low / len(pieces), top_value / len(pieces))
        return jnp.repeat(jnp.exp(heights), dims[axis_at] // parts).reshape((-1,) + (1,) * (len(dims) - axis_at - 1))

    level = one(*pieces[0])
    for cut in pieces[1:]:
        level = level * one(*cut)
    return level


def bell_draw(key, extent, scale, limit, cuts=(), kind=jnp.bfloat16):
    values = jax.random.normal(key, extent, jnp.float32) * scale
    if len(cuts) > 0:
        values = block_scale(key, extent, cuts, -0.22, 0.18) * values
    return jnp.clip(values, min=-limit, max=limit).astype(kind)


def setup_inputs(seed: int = 0) -> dict:
    seeds = jax.random.split(jax.random.key(seed), 8)
    old_master = bell_draw(seeds[0], (EXPERTS, ROWS, FF), 0.5, 3.0, ((0, 4), (1, 8)), jnp.float32)
    old_first = bell_draw(seeds[1], (EXPERTS, ROWS, FF), 0.5, 3.0, ((0, 4), (1, 8)), jnp.float32)
    old_second = jnp.clip(jnp.exp(math.log(1.0) - 4.6051702 * jax.random.uniform(seeds[2], (EXPERTS, ROWS, FF), jnp.float32) ** block_scale(seeds[2], (EXPERTS, ROWS, FF), ((0, 4), (1, 8)), -0.2, 0.2)), 0.01, 1.0)
    new_grad = bell_draw(seeds[3], (EXPERTS, ROWS, FF), (16 * EXPERTS), 3072.0, ((0, 32),))
    counts = draw_counts(jax.random.fold_in(seeds[7], 71), 0)
    old_owner = jax.random.permutation(seeds[5], EXPERTS).astype(jnp.int32)
    new_owner = jax.random.permutation(seeds[6], EXPERTS).astype(jnp.int32)
    return {"old_master": old_master, "old_first": old_first, "old_second": old_second, "new_grad": new_grad, "counts": counts, "old_owner": old_owner, "new_owner": new_owner}


first_correction = 1.0 - 0.9 ** 10
second_correction = 1.0 - 0.999 ** 10

def adam_step(master, first, second, grad, slot_count):
    scaled = grad.astype(jnp.float32) / slot_count
    new_first = 0.9 * first + 0.1 * scaled
    new_second = 0.999 * second + 0.001 * scaled * scaled
    step_dir = new_first / first_correction / (jnp.sqrt(new_second / second_correction) + 1e-08)
    new_master = master - 0.01 * (step_dir + 0.1 * master)
    return (new_master, new_first, new_second)

def reference(old_master, old_first, old_second, new_grad, counts, old_owner, new_owner):
    slots = jnp.arange(EXPERTS, dtype=jnp.int32)
    onehot = new_owner[:, None] == slots[None, :]
    source = lax.optimization_barrier(jnp.sum(jnp.where(onehot, old_owner[:, None], 0), axis=0)).astype(jnp.int32)
    totals = lax.optimization_barrier(jnp.sum(counts.astype(jnp.float32), axis=1))
    slot_count = lax.optimization_barrier(jnp.sum(jnp.where(onehot, totals[:, None], jnp.float32(0.0)), axis=0))
    master = jnp.take(old_master, source, axis=0)
    first = jnp.take(old_first, source, axis=0)
    second = jnp.take(old_second, source, axis=0)
    return adam_step(master, first, second, new_grad, slot_count[:, None, None])
```

```python
import functools

import jax
import jax.numpy as jnp
from jax import lax
from jax.experimental import pallas as pl
from jax.experimental.pallas import tpu as pltpu
from jax.sharding import PartitionSpec as P

first_correction = 1.0 - 0.9**10
second_correction = 1.0 - 0.999**10


VMEM = pltpu.VMEM
SMEM = pltpu.SMEM


def partner(index, step, size):
    if size & (size - 1) == 0:
        return index ^ step
    return (step - index) % size


def pick_kernel(n_parts, count, index_ref, *refs):
    parts, out_ref = refs[:n_parts], refs[n_parts]
    for k in range(count):
        i = index_ref[k]
        for j, part in enumerate(parts):

            @pl.when((i >= j * count) & (i < (j + 1) * count))
            def _():
                out_ref[k] = part[i - j * count]


def pick_split_kernel(n_parts, count, index_ref, *refs):
    parts, got, outs = refs[:n_parts], refs[n_parts], refs[n_parts + 1 :]
    for k in range(count):
        i = index_ref[k]

        @pl.when(i < 0)
        def _():
            outs[k][...] = got[k]

        for j, part in enumerate(parts):

            @pl.when((i >= j * count) & (i < (j + 1) * count))
            def _():
                outs[k][...] = part[i - j * count]


def adam_kernel(groups, rows, place_ref, count_ref, grad_ref, *refs):
    pieces = refs[: 3 * groups]
    master_out, first_out, second_out = refs[3 * groups :]
    slot_count = count_ref[0]
    for k in range(groups):
        here = pl.ds(pl.multiple_of(place_ref[k] * rows, rows), rows)
        master = pieces[k][...]
        first = pieces[groups + k][...]
        second = pieces[2 * groups + k][...]
        scaled = grad_ref[0, here, :].astype(jnp.float32) / slot_count
        new_first = 0.9 * first + 0.1 * scaled
        new_second = 0.999 * second + 0.001 * scaled * scaled
        step_dir = new_first / first_correction / (jnp.sqrt(new_second / second_correction) + 1e-08)
        master_out[0, here, :] = master - 0.01 * (step_dir + 0.1 * master)
        first_out[0, here, :] = new_first
        second_out[0, here, :] = new_second


def body(old_master, old_first, old_second, new_grad, counts, old_owner, new_owner):
    groups_x = lax.axis_size("gx")
    groups_y = lax.axis_size("gy")
    held, rows, width = old_master.shape
    cores = 2 if groups_x % 2 == 0 else 1
    chips = groups_x // cores
    x = lax.axis_index("gx")
    y = lax.axis_index("gy")
    chip, core = x // cores, x % cores

    order = jnp.stack([jnp.int32(partner(y, k, groups_y)) for k in range(groups_y)])

    def wanted(column):
        slots = column * groups_y + order
        onehot = new_owner[:, None] == slots[None, :]
        source = jnp.sum(jnp.where(onehot, old_owner[:, None], 0), axis=0)
        from_x = source // held
        lag = (chip - from_x // cores + chips) % chips
        return jnp.where(from_x % cores == core, lag * held + source % held, -1)

    index_mine = wanted(x)
    other_x = chip * cores + (cores - 1 - core)
    index_other = wanted(other_x)

    across = [
        [(i, ((i // cores + d) % chips) * cores + i % cores) for i in range(groups_x)]
        for d in range(1, chips)
    ]
    swap = [(i, (i // cores) * cores + (cores - 1 - i % cores)) for i in range(groups_x)]
    vm = pl.BlockSpec(memory_space=VMEM)
    sm = pl.BlockSpec(memory_space=SMEM)

    tally = counts[:, 0].astype(jnp.float32)
    near = tally
    for pairs in across:
        near = near + lax.ppermute(tally, "gx", pairs)
    if cores == 2:
        near = near + lax.ppermute(near, "gx", swap)
    step = 1
    if groups_y & (groups_y - 1) == 0:
        while step < groups_y:
            near = near + lax.ppermute(near, "gy", [(i, i ^ step) for i in range(groups_y)])
            step *= 2
        totals = near
    else:
        totals = lax.psum(near, "gy")
    my_slot = x * groups_y + y
    slot_count = jnp.sum(jnp.where(new_owner == my_slot, totals, jnp.float32(0.0)))

    pieces = []
    for state in (old_master, old_first, old_second):
        parts = [state] + [lax.ppermute(state, "gx", pairs) for pairs in across]
        if cores == 2:
            chosen = pl.pallas_call(
                functools.partial(pick_kernel, chips, held),
                out_shape=jax.ShapeDtypeStruct((held, rows, width), jnp.float32),
                in_specs=[sm] + [vm] * chips,
                out_specs=vm,
            )(index_other, *parts)
            got = lax.ppermute(chosen, "gx", swap)
        else:
            got = state
        ready = pl.pallas_call(
            functools.partial(pick_split_kernel, chips, held),
            out_shape=[jax.ShapeDtypeStruct((rows, width), jnp.float32)] * held,
            in_specs=[sm] + [vm] * (chips + 1),
            out_specs=[vm] * held,
        )(index_mine, *parts, got)
        for k in range(groups_y):
            pairs = [(i, partner(i, k, groups_y)) for i in range(groups_y)]
            pieces.append(ready[k] if all(a == b for a, b in pairs) else lax.ppermute(ready[k], "gy", pairs))

    out = jax.ShapeDtypeStruct(new_grad.shape, jnp.float32)
    return tuple(
        pl.pallas_call(
            functools.partial(adam_kernel, groups_y, rows),
            out_shape=[out] * 3,
            in_specs=[sm, sm, vm] + [vm] * (3 * groups_y),
            out_specs=[vm] * 3,
        )(order, slot_count.reshape(1), new_grad, *pieces)
    )


def solution(mesh):
    placed = (
        P("gx", "gy", None),
        P("gx", "gy", None),
        P("gx", "gy", None),
        P(("gx", "gy"), None, None),
        P(None, ("gx", "gy")),
        P(),
        P(),
    )
    return jax.shard_map(
        body,
        mesh=mesh,
        in_specs=placed,
        out_specs=(
            P(("gx", "gy"), None, None),
            P(("gx", "gy"), None, None),
            P(("gx", "gy"), None, None),
        ),
        check_vma=False,
    )
```

```python
import jax
import jax.numpy as jnp
from jax import lax
from jax.experimental import pallas as pl
from jax.experimental.pallas import tpu as pltpu
from jax.sharding import PartitionSpec as P


first_correction = 1.0 - 0.9**10
second_correction = 1.0 - 0.999**10


def partner(index, step, size):
    if size & (size - 1) == 0:
        return index ^ step
    return (step - index) % size


def adam_kernel(place_ref, count_ref, grad_ref, piece_ref, *refs):
    master_out, first_out, second_out = refs[-3:]
    slot_count = count_ref[0]
    master = piece_ref[0]
    first = piece_ref[1]
    second = piece_ref[2]
    scaled = grad_ref[0].astype(jnp.float32) / slot_count
    new_first = 0.9 * first + 0.1 * scaled
    new_second = 0.999 * second + 0.001 * scaled * scaled
    step_dir = new_first / first_correction / (jnp.sqrt(new_second / second_correction) + 1e-08)
    master_out[0] = master - 0.01 * (step_dir + 0.1 * master)
    first_out[0] = new_first
    second_out[0] = new_second


def adam_chunk(place, slot_count, grad, piece, carried):
    _, rows, width = piece.shape
    out = jax.ShapeDtypeStruct(grad.shape, jnp.float32)
    spot = pl.BlockSpec((1, rows, width), lambda i, place_ref, count_ref: (0, place_ref[0], 0))
    whole = pl.BlockSpec((3, rows, width), lambda i, place_ref, count_ref: (0, 0, 0))
    apart = pl.BlockSpec(memory_space=pl.ANY)
    return pl.pallas_call(
        adam_kernel,
        grid_spec=pltpu.PrefetchScalarGridSpec(
            num_scalar_prefetch=2,
            grid=(1,),
            in_specs=[spot, whole] + [apart] * len(carried),
            out_specs=[spot] * 3,
        ),
        out_shape=[out] * 3,
        input_output_aliases={4 + j: j for j in range(len(carried))},
        compiler_params=pltpu.CompilerParams(vmem_limit_bytes=8 * 1024 * 1024),
    )(place, slot_count, grad, piece, *carried)


def body(order_k, old_master, old_first, old_second, new_grad, counts, old_owner, new_owner):
    groups_x = lax.axis_size("gx")
    groups_y = lax.axis_size("gy")
    held, _, _ = old_master.shape
    cores = 2 if groups_x % 2 == 0 else 1
    chips = groups_x // cores
    x = lax.axis_index("gx")
    y = lax.axis_index("gy")
    chip, core = x // cores, x % cores
    swap = [(i, (i // cores) * cores + (cores - 1 - i % cores)) for i in range(groups_x)]
    across = [
        [(i, ((i // cores + d) % chips) * cores + i % cores) for i in range(groups_x)]
        for d in range(1, chips)
    ]
    order = [jnp.int32(partner(y, k, groups_y)) for k in range(groups_y)]

    own = (old_master, old_first, old_second)
    if cores == 2:
        near = tuple(lax.ppermute(state, "gx", swap) for state in own)
    else:
        near = own

    columns = jnp.stack([((chip + d) % chips) * cores + core for d in range(chips)])
    slots = columns[:, None] * groups_y + jnp.stack(order)[None, :]
    onehot = new_owner[:, None, None] == slots[None]
    source = jnp.sum(jnp.where(onehot, old_owner[:, None, None], 0), axis=0)
    from_x, spot = source // held, source % held
    is_own = from_x % cores == core
    lag = (chip - from_x // cores + chips) % chips

    def held_piece(d, k):
        picked = [
            jnp.where(
                is_own[d, k],
                lax.dynamic_index_in_dim(a, spot[d, k], 0),
                lax.dynamic_index_in_dim(b, spot[d, k], 0),
            )
            for a, b in zip(own, near)
        ]
        return jnp.concatenate(picked, axis=0)

    tally = counts[:, 0].astype(jnp.float32)
    for pairs in across:
        tally = tally + lax.ppermute(counts[:, 0].astype(jnp.float32), "gx", pairs)
    if cores == 2:
        tally = tally + lax.ppermute(tally, "gx", swap)
    if groups_y & (groups_y - 1) == 0:
        step = 1
        while step < groups_y:
            tally = tally + lax.ppermute(tally, "gy", [(i, i ^ step) for i in range(groups_y)])
            step *= 2
    else:
        tally = lax.psum(tally, "gy")
    my_slot = x * groups_y + y
    slot_count = jnp.sum(jnp.where(new_owner == my_slot, tally, jnp.float32(0.0))).reshape(1)

    ready = {}
    for k in order_k:
        sent = []
        for d in range(1, chips):
            chosen = held_piece(d, k)
            sent.append(lax.ppermute(chosen, "gx", across[d - 1]))
        piece = held_piece(0, k)
        for d in range(1, chips):
            piece = jnp.where(lag[0, k] == d, sent[d - 1], piece)
        pairs = [(i, partner(i, k, groups_y)) for i in range(groups_y)]
        if any(a != b for a, b in pairs):
            piece = lax.ppermute(piece, "gy", pairs)
        ready[k] = piece

    carried = ()
    for k in order_k[-1:] + order_k[:-1]:
        carried = adam_chunk(order[k].reshape(1), slot_count, new_grad, ready[k], carried)
    return tuple(carried)


def solution(mesh):
    groups_y = mesh.shape["gy"]
    order_k = list(range(groups_y // 2, groups_y)) + list(range(groups_y // 2 - 1, -1, -1))

    def stepped(*args):
        return body(order_k, *args)

    placed = (
        P("gx", "gy", None),
        P("gx", "gy", None),
        P("gx", "gy", None),
        P(("gx", "gy"), None, None),
        P(None, ("gx", "gy")),
        P(),
        P(),
    )
    return jax.shard_map(
        stepped,
        mesh=mesh,
        in_specs=placed,
        out_specs=(
            P(("gx", "gy"), None, None),
            P(("gx", "gy"), None, None),
            P(("gx", "gy"), None, None),
        ),
        check_vma=False,
    )
```

```python
import functools

import jax
import jax.numpy as jnp
from jax import lax
from jax.experimental import pallas as pl
from jax.experimental.pallas import tpu as pltpu
from jax.sharding import PartitionSpec as P


first_correction = 1.0 - 0.9**10
second_correction = 1.0 - 0.999**10

MIB = 1024 * 1024
LOAD_MIB, MERGE_MIB, ADAM_MIB = 12, 2, 8


def partner(index, step, size):
    if size & (size - 1) == 0:
        return index ^ step
    return (step - index) % size


def load_kernel(chips, count, pick_ref, *refs):
    own, near, outs = refs[:3], refs[3:6], refs[6:]
    for d in range(chips):
        for k in range(count):
            at = pick_ref[d * count + k]
            out = outs[d * count + k]

            @pl.when(at < count)
            def _():
                for j in range(3):
                    out[j] = own[j][at]

            @pl.when(at >= count)
            def _():
                for j in range(3):
                    out[j] = near[j][at - count]


def merge_kernel(chips, lag_ref, *refs):
    out_ref = refs[-1]
    for d in range(chips):

        @pl.when(lag_ref[0] == d)
        def _():
            out_ref[...] = refs[d][...]


def adam_kernel(groups, rows, place_ref, count_ref, grad_ref, *refs):
    pieces = refs[:groups]
    master_out, first_out, second_out = refs[groups:]
    slot_count = count_ref[0]
    for k in range(groups):
        here = pl.ds(pl.multiple_of(place_ref[k] * rows, rows), rows)
        master = pieces[k][0]
        first = pieces[k][1]
        second = pieces[k][2]
        scaled = grad_ref[0, here, :].astype(jnp.float32) / slot_count
        new_first = 0.9 * first + 0.1 * scaled
        new_second = 0.999 * second + 0.001 * scaled * scaled
        step_dir = new_first / first_correction / (jnp.sqrt(new_second / second_correction) + 1e-08)
        master_out[0, here, :] = master - 0.01 * (step_dir + 0.1 * master)
        first_out[0, here, :] = new_first
        second_out[0, here, :] = new_second


def body(order_k, old_master, old_first, old_second, new_grad, counts, old_owner, new_owner):
    groups_x = lax.axis_size("gx")
    groups_y = lax.axis_size("gy")
    held, rows, width = old_master.shape
    cores = 2 if groups_x % 2 == 0 else 1
    chips = groups_x // cores
    x = lax.axis_index("gx")
    y = lax.axis_index("gy")
    chip, core = x // cores, x % cores
    swap = [(i, (i // cores) * cores + (cores - 1 - i % cores)) for i in range(groups_x)]
    across = [
        [(i, ((i // cores + d) % chips) * cores + i % cores) for i in range(groups_x)]
        for d in range(1, chips)
    ]
    vm = pl.BlockSpec(memory_space=pltpu.VMEM)
    sm = pl.BlockSpec(memory_space=pltpu.SMEM)

    own = (old_master, old_first, old_second)
    if cores == 2:
        near = tuple(lax.ppermute(state, "gx", swap) for state in own)
    else:
        near = own

    step_k = jnp.array(order_k, dtype=jnp.int32)
    order = partner(y, step_k, groups_y)
    shift = jnp.arange(chips, dtype=jnp.int32)
    columns = ((chip + shift) % chips) * cores + core
    slots = columns[:, None] * groups_y + order[None, :]
    onehot = new_owner[:, None, None] == slots[None]
    source = jnp.sum(jnp.where(onehot, old_owner[:, None, None], 0), axis=0)
    from_x = source // held
    pick = source % held + jnp.where(from_x % cores == core, 0, held)
    lag = (chip - from_x[0] // cores + chips) % chips

    tally = counts[:, 0].astype(jnp.float32)
    for pairs in across:
        tally = tally + lax.ppermute(counts[:, 0].astype(jnp.float32), "gx", pairs)
    if cores == 2:
        tally = tally + lax.ppermute(tally, "gx", swap)

    piece = jax.ShapeDtypeStruct((3, rows, width), jnp.float32)
    loaded = list(pl.pallas_call(
        functools.partial(load_kernel, chips, held),
        out_shape=[piece] * (chips * held),
        in_specs=[sm] + [vm] * 6,
        out_specs=[vm] * (chips * held),
        compiler_params=pltpu.CompilerParams(vmem_limit_bytes=LOAD_MIB * MIB),
    )(pick.reshape(-1), *own, *near))

    tally, loaded[0] = lax.optimization_barrier((tally, loaded[0]))
    if groups_y & (groups_y - 1) == 0:
        step = 1
        while step < groups_y:
            tally = tally + lax.ppermute(tally, "gy", [(i, i ^ step) for i in range(groups_y)])
            step *= 2
    else:
        tally = lax.psum(tally, "gy")
    my_slot = x * groups_y + y
    slot_count = jnp.sum(jnp.where(new_owner == my_slot, tally, jnp.float32(0.0))).reshape(1)

    arrived = []
    for n, k in enumerate(order_k):
        sent = []
        for d in range(1, chips):
            sent.append(lax.ppermute(loaded[d * held + n], "gx", across[d - 1]))
        merged = pl.pallas_call(
            functools.partial(merge_kernel, chips),
            out_shape=piece,
            in_specs=[sm] + [vm] * chips,
            out_specs=vm,
            compiler_params=pltpu.CompilerParams(vmem_limit_bytes=MERGE_MIB * MIB),
        )(lax.dynamic_slice_in_dim(lag, n, 1), loaded[n], *sent)
        pairs = [(i, partner(i, k, groups_y)) for i in range(groups_y)]
        if any(a != b for a, b in pairs):
            merged = lax.ppermute(merged, "gy", pairs)
        arrived.append(merged)

    out = jax.ShapeDtypeStruct(new_grad.shape, jnp.float32)
    return tuple(
        pl.pallas_call(
            functools.partial(adam_kernel, groups_y, rows),
            out_shape=[out] * 3,
            in_specs=[sm, sm, vm] + [vm] * groups_y,
            out_specs=[vm] * 3,
            compiler_params=pltpu.CompilerParams(vmem_limit_bytes=ADAM_MIB * MIB),
        )(order, slot_count, new_grad, *arrived)
    )


def solution(mesh):
    groups_y = mesh.shape["gy"]
    half = groups_y // 2
    order_k = list(range(1, half)) + list(range(groups_y - 1, half - 1, -1)) + [0]

    def stepped(*args):
        return body(order_k, *args)

    placed = (
        P("gx", "gy", None),
        P("gx", "gy", None),
        P("gx", "gy", None),
        P(("gx", "gy"), None, None),
        P(None, ("gx", "gy")),
        P(),
        P(),
    )
    return jax.shard_map(
        stepped,
        mesh=mesh,
        in_specs=placed,
        out_specs=(
            P(("gx", "gy"), None, None),
            P(("gx", "gy"), None, None),
            P(("gx", "gy"), None, None),
        ),
        check_vma=False,
    )
```

```python
import functools

import jax
import jax.numpy as jnp
from jax import lax
from jax.experimental import pallas as pl
from jax.experimental.pallas import tpu as pltpu
from jax.sharding import PartitionSpec as P


first_correction = 1.0 - 0.9**10
second_correction = 1.0 - 0.999**10

MIB = 1024 * 1024
LOAD_MIB, MERGE_MIB, ADAM_MIB = 12, 2, 8


def partner(index, step, size):
    if size & (size - 1) == 0:
        return index ^ step
    return (step - index) % size


def load_kernel(chips, count, pick_ref, *refs):
    own, near, outs = refs[:3], refs[3:6], refs[6:]
    for d in range(chips):
        for k in range(count):
            at = pick_ref[d * count + k]
            out = outs[d * count + k]

            @pl.when(at < count)
            def _():
                for j in range(3):
                    out[j] = own[j][at]

            @pl.when(at >= count)
            def _():
                for j in range(3):
                    out[j] = near[j][at - count]


def merge_kernel(chips, lag_ref, *refs):
    out_ref = refs[-1]
    for d in range(chips):

        @pl.when(lag_ref[0] == d)
        def _():
            out_ref[...] = refs[d][...]


def adam_kernel(groups, rows, place_ref, count_ref, grad_ref, *refs):
    pieces = refs[:groups]
    master_out, first_out, second_out = refs[groups:]
    slot_count = count_ref[0]
    for k in range(groups):
        here = pl.ds(pl.multiple_of(place_ref[k] * rows, rows), rows)
        master = pieces[k][0]
        first = pieces[k][1]
        second = pieces[k][2]
        scaled = grad_ref[0, here, :].astype(jnp.float32) / slot_count
        new_first = 0.9 * first + 0.1 * scaled
        new_second = 0.999 * second + 0.001 * scaled * scaled
        step_dir = new_first / first_correction / (jnp.sqrt(new_second / second_correction) + 1e-08)
        master_out[0, here, :] = master - 0.01 * (step_dir + 0.1 * master)
        first_out[0, here, :] = new_first
        second_out[0, here, :] = new_second


def body(order_k, old_master, old_first, old_second, new_grad, counts, old_owner, new_owner):
    groups_x = lax.axis_size("gx")
    groups_y = lax.axis_size("gy")
    held, rows, width = old_master.shape
    cores = 2 if groups_x % 2 == 0 else 1
    chips = groups_x // cores
    x = lax.axis_index("gx")
    y = lax.axis_index("gy")
    chip, core = x // cores, x % cores
    swap = [(i, (i // cores) * cores + (cores - 1 - i % cores)) for i in range(groups_x)]
    across = [
        [(i, ((i // cores + d) % chips) * cores + i % cores) for i in range(groups_x)]
        for d in range(1, chips)
    ]
    vm = pl.BlockSpec(memory_space=pltpu.VMEM)
    sm = pl.BlockSpec(memory_space=pltpu.SMEM)

    own = (old_master, old_first, old_second)
    if cores == 2:
        near = tuple(lax.ppermute(state, "gx", swap) for state in own)
    else:
        near = own

    step_k = jnp.array(order_k, dtype=jnp.int32)
    order = partner(y, step_k, groups_y)
    shift = jnp.arange(chips, dtype=jnp.int32)
    columns = ((chip + shift) % chips) * cores + core
    slots = columns[:, None] * groups_y + order[None, :]
    onehot = new_owner[:, None, None] == slots[None]
    source = jnp.sum(jnp.where(onehot, old_owner[:, None, None], 0), axis=0)
    from_x = source // held
    pick = source % held + jnp.where(from_x % cores == core, 0, held)
    lag = (chip - from_x[0] // cores + chips) % chips

    tally = counts[:, 0].astype(jnp.float32)
    for pairs in across:
        tally = tally + lax.ppermute(counts[:, 0].astype(jnp.float32), "gx", pairs)
    if cores == 2:
        tally = tally + lax.ppermute(tally, "gx", swap)

    piece = jax.ShapeDtypeStruct((3, rows, width), jnp.float32)
    loaded = list(pl.pallas_call(
        functools.partial(load_kernel, chips, held),
        out_shape=[piece] * (chips * held),
        in_specs=[sm] + [vm] * 6,
        out_specs=[vm] * (chips * held),
        compiler_params=pltpu.CompilerParams(vmem_limit_bytes=LOAD_MIB * MIB),
    )(pick.reshape(-1), *own, *near))

    tally, loaded[0] = lax.optimization_barrier((tally, loaded[0]))
    if groups_y & (groups_y - 1) == 0:
        for hop in range(groups_y.bit_length() - 1):
            pairs = [(i, i ^ (1 << hop)) for i in range(groups_y)]
            tally = tally + lax.ppermute(tally, "gy", pairs)
    else:
        tally = lax.psum(tally, "gy")
    my_slot = x * groups_y + y
    slot_count = jnp.sum(jnp.where(new_owner == my_slot, tally, jnp.float32(0.0))).reshape(1)

    arrived = []
    for n, k in enumerate(order_k):
        sent = []
        for d in range(1, chips):
            sent.append(lax.ppermute(loaded[d * held + n], "gx", across[d - 1]))
        merged = pl.pallas_call(
            functools.partial(merge_kernel, chips),
            out_shape=piece,
            in_specs=[sm] + [vm] * chips,
            out_specs=vm,
            compiler_params=pltpu.CompilerParams(vmem_limit_bytes=MERGE_MIB * MIB),
        )(lax.dynamic_slice_in_dim(lag, n, 1), loaded[n], *sent)
        pairs = [(i, partner(i, k, groups_y)) for i in range(groups_y)]
        if any(a != b for a, b in pairs):
            merged = lax.ppermute(merged, "gy", pairs)
        arrived.append(merged)

    out = jax.ShapeDtypeStruct(new_grad.shape, jnp.float32)
    return tuple(
        pl.pallas_call(
            functools.partial(adam_kernel, groups_y, rows),
            out_shape=[out] * 3,
            in_specs=[sm, sm, vm] + [vm] * groups_y,
            out_specs=[vm] * 3,
            compiler_params=pltpu.CompilerParams(vmem_limit_bytes=ADAM_MIB * MIB),
        )(order, slot_count, new_grad, *arrived)
    )


def solution(mesh):
    groups_y = mesh.shape["gy"]
    half = groups_y // 2
    order_k = list(range(1, half)) + list(range(groups_y - 1, half - 1, -1)) + [0]

    def stepped(*args):
        return body(order_k, *args)

    placed = (
        P("gx", "gy", None),
        P("gx", "gy", None),
        P("gx", "gy", None),
        P(("gx", "gy"), None, None),
        P(None, ("gx", "gy")),
        P(),
        P(),
    )
    return jax.shard_map(
        stepped,
        mesh=mesh,
        in_specs=placed,
        out_specs=(
            P(("gx", "gy"), None, None),
            P(("gx", "gy"), None, None),
            P(("gx", "gy"), None, None),
        ),
        check_vma=False,
    )
```
